32 devices in a mesh: grp: 8 (over z, x), sub: 4 (over y, core).
Axes of the slice: x: 2, y: 2, z: 4, core: 2. Of those that a mesh axis runs over, the one named last changes fastest.
Arguments:
- gate_source: bfloat16 [32, 2048, 768], P('grp', 'sub'), may hold values from -0.125 to 0.125
- up_source: bfloat16 [32, 2048, 768], P('grp', 'sub'), may hold values from -0.125 to 0.125
- down_source: bfloat16 [32, 2048, 768], P('grp', 'sub'), may hold values from -0.21875 to 0.21875
- source_order: int32 [32], replicated, may hold values from 0 to 31, each once
- target_order: int32 [32], replicated, may hold values from 0 to 31, each once
Outputs:
- packed: bfloat16 [3, 8, 4, 8, 96, 2048], P(None, 'grp', 'sub')
- scales: float32 [3, 8, 4, 16, 768], P(None, 'grp', 'sub')
The draws below stay inside these ranges and needn't reach their ends.
Inputs may be any that keep to these rules, and one draw needn't show every extreme that they name: `source_order`: each expert number appears once. `target_order`: each expert number appears once.
All inputs are finite; a program needn't handle non-finite values. Where the reference program divides by a largest or mean magnitude, that divisor is 1e-20 or more.
Results may differ from the reference program's by a relative error of at most 0.001.
Values may be sent and summed in bfloat16 or wider, within the bound.
A program may use at most 192 MiB of HBM per device.

```python
import jax
import jax.numpy as jnp
from jax import lax

D = 2048
FF = 768
BLOCK = 128
E = 32
EPT = 8
FFT = 96
N_GRP = 8
N_SUB = 4


def levels(rng, shape, shards, smallest, largest):
    def one(position, blocks):
        steps = jax.random.uniform(jax.random.fold_in(jax.random.fold_in(rng, 6), position), (blocks,), jnp.float32, smallest / len(shards), largest / len(shards))
        return jnp.repeat(jnp.exp(steps), shape[position] // blocks).reshape((-1,) + (1,) * (len(shape) - position - 1))

    level = one(*shards[0])
    for cut in shards[1:]:
        level = level * one(*cut)
    return level


def bell_draw(own_key, shape, spread, most, cuts=(), kind=jnp.bfloat16):
    entries = spread * jax.random.normal(own_key, shape, jnp.float32)
    if cuts:
        entries = entries * levels(own_key, shape, cuts, -0.22, 0.18)
    return jnp.clip(entries, -most, most).astype(kind)


def setup_inputs(seed: int = 0) -> dict:
    splits = jax.random.split(jax.random.key(seed), 6)
    return {
        "gate_source": bell_draw(splits[0], (E, D, FF), D ** -0.5, 0.125, ((0, 8), (1, 4))),
        "up_source": bell_draw(splits[1], (E, D, FF), D ** -0.5, 0.125, ((0, 8), (1, 4))),
        "down_source": bell_draw(splits[2], (E, D, FF), FF ** -0.5, 0.21875, ((0, 8), (1, 4))),
        "source_order": jax.random.permutation(splits[3], E).astype(jnp.int32),
        "target_order": jax.random.permutation(splits[4], E).astype(jnp.int32),
    }


EPS = 1e-6


def pack_layout(quantized):
    values = quantized.reshape(N_GRP // 2, EPT, D, 2, N_SUB, FFT)
    values = values.transpose(0, 3, 4, 1, 5, 2)
    return values.reshape(N_GRP, N_SUB, EPT, FFT, D)


def scale_layout(block_scale):
    values = block_scale.reshape(N_GRP // 2, EPT, D // BLOCK, 2, N_SUB, FFT)
    values = values.transpose(0, 3, 4, 2, 1, 5)
    return values.reshape(N_GRP, N_SUB, D // BLOCK, EPT * FFT)


def convert(weights, picked):
    def convert_one(target):
        matrix = weights[picked[target]].astype(jnp.float32).reshape(D // BLOCK, BLOCK, FF)
        block_scale = jnp.max(jnp.abs(matrix), axis=1) + EPS
        quantized = (matrix / block_scale[:, None, :]).astype(jnp.bfloat16).reshape(D, FF)
        return quantized, block_scale

    quantized, block_scale = lax.map(convert_one, jnp.arange(E, dtype=jnp.int32))
    return pack_layout(quantized), scale_layout(block_scale)


def reference(gate_source, up_source, down_source, source_order, target_order):
    matches = (source_order[None, :] == target_order[:, None]).astype(jnp.int32)
    picked = jnp.sum(matches * jnp.arange(E, dtype=jnp.int32)[None, :], axis=1).astype(jnp.int32)
    gate_q, gate_s = convert(gate_source, picked)
    up_q, up_s = convert(up_source, picked)
    down_q, down_s = convert(down_source, picked)
    return jnp.stack([gate_q, up_q, down_q]), jnp.stack([gate_s, up_s, down_s])
```

```python
import functools

import jax
import jax.numpy as jnp
from jax import lax
from jax.experimental import pallas as pl
from jax.experimental.pallas import tpu as pltpu
from jax.sharding import PartitionSpec as P

BLOCK = 128
EPS = 1e-06
MESH = pl.DeviceIdType.MESH
PIECE = 16
CAPS = (7, 8, 9, 10)
LOADS = 3
TURNS = 4
RING = 4
AHEAD = 2
LAG_IN = 2
LAG_OUT = 6


def pick(source_order, target_order):
    matches = source_order[None, :] == target_order[:, None]
    slots = jnp.arange(source_order.shape[0], dtype=jnp.int32)
    return jnp.sum(jnp.where(matches, slots[None, :], 0), axis=1, dtype=jnp.int32)


def plain(gate_source, up_source, down_source, source_order, target_order):
    stacked = jnp.stack([gate_source, up_source, down_source])
    matrices, local_slots, local_rows, hidden = stacked.shape
    groups = lax.axis_size("grp")
    shards = lax.axis_size("sub")
    devices = groups * shards
    experts = local_slots * groups
    full_rows = local_rows * shards
    targets = groups // 2
    per_group = experts // targets
    splits = 2 * shards
    columns = hidden // splits
    picked = pick(source_order, target_order)
    slab_rows = local_rows // devices
    pieces = stacked.reshape(matrices, 1, local_slots, devices, slab_rows, hidden)
    received = lax.all_to_all(pieces, ("grp", "sub"), split_axis=3, concat_axis=1, tiled=True)
    received = received.reshape(matrices, groups, shards, local_slots, slab_rows, hidden)
    received = received.transpose(0, 1, 3, 2, 4, 5).reshape(
        matrices, experts, shards * slab_rows, hidden
    )
    ordered = jnp.take(received, picked, axis=1)
    outgoing = ordered.reshape(matrices, targets, per_group, shards * slab_rows, splits, columns)
    outgoing = outgoing.transpose(0, 1, 4, 2, 3, 5).reshape(
        matrices, devices, per_group, 1, shards * slab_rows, columns
    )
    placed = lax.all_to_all(outgoing, ("grp", "sub"), split_axis=1, concat_axis=3, tiled=True)
    placed = placed.reshape(matrices, per_group, devices, shards, slab_rows, columns)
    placed = placed.transpose(0, 1, 3, 2, 4, 5).reshape(matrices, per_group, full_rows, columns)
    num_blocks = full_rows // BLOCK
    blocks = placed.astype(jnp.float32).reshape(matrices, per_group, num_blocks, BLOCK, columns)
    block_scale = jnp.max(jnp.abs(blocks), axis=3) + EPS
    quantized = (blocks / block_scale[:, :, :, None, :]).astype(jnp.bfloat16)
    quantized = quantized.reshape(matrices, per_group, full_rows, columns).transpose(0, 1, 3, 2)
    quantized = quantized.reshape(matrices, 1, 1, per_group, columns, full_rows)
    block_scale = block_scale.transpose(0, 2, 1, 3).reshape(
        matrices, 1, 1, num_blocks, per_group * columns
    )
    return (quantized, block_scale)


def plan_kernel(per_zone, source_order, target_order, table, choice, goes):
    experts = source_order.shape[0]
    spare = table.shape[0] - 1
    zone = lax.axis_index("grp") // 2
    i32 = jnp.int32

    def outer(z):
        return (z == 0) | (z == 3)

    def clear(i, _):
        table[i] = 0
        return 0

    lax.fori_loop(0, spare + 1, clear, 0)

    def note(j, _):
        goes[target_order[j]] = j
        return 0

    lax.fori_loop(0, experts, note, 0)

    def route(p, counts):
        in0, in3, mid0, mid1, out0, out3 = counts
        target = goes[source_order[p]]
        here, there, own = p // per_zone, target // per_zone, p % per_zone
        moves = here != there
        leaves = outer(here) & moves
        crosses = (here // 2) != (there // 2)
        enters = outer(there) & moves
        rank_in = jnp.where(here == 0, in0, in3)
        rank_mid = jnp.where(here < 2, mid0, mid1)
        rank_out = jnp.where(there == 0, out0, out3)
        on_inner = jnp.where(leaves, per_zone + rank_in, own)
        after_mid = jnp.where(crosses, 2 * per_zone + rank_mid, on_inner)
        last = jnp.where(moves, jnp.where(outer(there), per_zone + rank_out, after_mid), own)
        inward = leaves & (here == zone)
        table[jnp.where(inward, rank_in, spare)] = own
        outward = enters & jnp.logical_not(outer(zone)) & ((there // 2) == (zone // 2))
        table[jnp.where(outward, rank_out, spare)] = after_mid
        over = crosses & ((here // 2) == (zone // 2))
        table[jnp.where(over, per_zone + rank_mid, spare)] = on_inner
        stays = there == zone
        table[jnp.where(stays, 3 * per_zone + target % per_zone, spare)] = last

        def add(flag):
            return jnp.where(flag, 1, 0).astype(i32)

        return (
            in0 + add(leaves & (here == 0)),
            in3 + add(leaves & (here == 3)),
            mid0 + add(crosses & (here < 2)),
            mid1 + add(crosses & (here >= 2)),
            out0 + add(enters & (there == 0)),
            out3 + add(enters & (there == 3)),
        )

    zero = jnp.zeros((), i32)
    in0, in3, mid0, _, _, _ = lax.fori_loop(0, experts, route, (zero,) * 6)
    load = jnp.maximum(mid0, jnp.maximum(in0, in3))
    index = zero
    for cap in CAPS:
        index = index + jnp.where(load > cap, 1, 0).astype(i32)
    choice[0] = index


def plan(source_order, target_order, per_zone):
    smem = pl.BlockSpec(memory_space=pltpu.SMEM)
    return pl.pallas_call(
        functools.partial(plan_kernel, per_zone),
        out_shape=(
            jax.ShapeDtypeStruct((4 * per_zone + 1,), jnp.int32),
            jax.ShapeDtypeStruct((1,), jnp.int32),
        ),
        in_specs=[smem, smem],
        out_specs=(smem, smem),
        scratch_shapes=[pltpu.SMEM(source_order.shape, jnp.int32)],
        name="plan",
    )(source_order, target_order)


def line_kernel(cap, per_zone, table, *refs):
    sources, out, kept = refs[:3], refs[3], refs[4]
    raw, turned, held, beside, middle, near, whole = refs[5:12]
    in_sem, ex_send, ex_recv, be_send, be_recv, mi_send, mi_recv = refs[12:]
    grp, sub = lax.axis_index("grp"), lax.axis_index("sub")
    zone, half = grp // 2, grp % 2
    matrices = len(sources)
    local, rows, hidden = sources[0].shape
    steps, _, shards, piece, _ = held.shape
    edge = beside.shape[1]
    splits = 2 * shards
    columns = hidden // splits
    cuts = columns // piece
    parts = rows // BLOCK
    chunks = matrices * parts
    me = half * shards + sub
    is_outer = (zone == 0) | (zone == 3)
    is_inner = (zone == 1) | (zone == 2)
    neighbour = (zone + 1 - 2 * (zone % 2)) * 2 + half
    across = (3 - zone) * 2 + half

    def load(g, i):
        return pltpu.make_async_copy(
            sources[i].at[:, pl.ds(pl.multiple_of((g % parts) * BLOCK, BLOCK), BLOCK), :],
            raw.at[g % LOADS],
            in_sem.at[g % LOADS],
        )

    def start_load(g):
        for i in range(matrices):

            @pl.when(g // parts == i)
            def _():
                load(g, i).start()

    def exchange(g, c, to):
        start = pl.multiple_of(to * columns + c * piece, 16)
        return pltpu.make_async_remote_copy(
            src_ref=turned.at[g % TURNS, :, pl.ds(start, piece), :],
            dst_ref=held.at[g * cuts + c, pl.ds(half * local, local), sub],
            send_sem=ex_send.at[g % TURNS],
            recv_sem=ex_recv.at[g * cuts + c],
            device_id=(zone * 2 + to // shards, to % shards),
            device_id_type=MESH,
        )

    def turn(g):
        load(g, 0).wait()

        def one(e, _):
            for b in range(hidden // BLOCK):
                turned[g % TURNS, e, b * BLOCK : (b + 1) * BLOCK, :] = raw[
                    g % LOADS, e, :, b * BLOCK : (b + 1) * BLOCK
                ].T
            return 0

        lax.fori_loop(0, local, one, 0)

        @pl.when(g + LOADS < chunks)
        def _():
            start_load(g + LOADS)

    def start_exchange(g):
        def cut(c, _):
            start = pl.multiple_of(me * columns + c * piece, 16)
            pltpu.make_async_copy(
                turned.at[g % TURNS, :, pl.ds(start, piece), :],
                held.at[g * cuts + c, pl.ds(half * local, local), sub],
                ex_recv.at[g * cuts + c],
            ).start()

            def go(d, _):
                exchange(g, c, lax.rem(me + d, splits)).start()
                return 0

            return lax.fori_loop(1, splits, go, 0)

        lax.fori_loop(0, cuts, cut, 0)

    def wait_exchange(j):
        mine = held.at[j, pl.ds(0, per_zone)]
        pltpu.make_async_copy(mine, mine, ex_recv.at[j]).wait()

    def gather(j, count, work):
        def one(i, _):
            work[i] = held[j, i]
            return 0

        lax.fori_loop(0, count, one, 0)

    def wait_turned(slot):
        sent = turned.at[slot, :, pl.ds(0, (splits - 1) * columns), :]
        pltpu.make_async_copy(sent, sent, ex_send.at[slot]).wait()

    def send_beside(j):
        return pltpu.make_async_remote_copy(
            src_ref=beside.at[j % RING], dst_ref=held.at[j, pl.ds(per_zone, edge)],
            send_sem=be_send.at[j % RING], recv_sem=be_recv.at[j],
            device_id=(neighbour, sub), device_id_type=MESH,
        )

    def send_middle(j):
        return pltpu.make_async_remote_copy(
            src_ref=middle.at[j % RING], dst_ref=held.at[j, pl.ds(2 * per_zone, cap)],
            send_sem=mi_send.at[j % RING], recv_sem=mi_recv.at[j],
            device_id=(across, sub), device_id_type=MESH,
        )

    def put_beside(j, work):
        @pl.when(j >= RING)
        def _():
            send_beside(j - RING).wait_send()

        def put(k, _):
            beside[j % RING, k] = work[table[k]]
            return 0

        lax.fori_loop(0, edge, put, 0)
        send_beside(j).start()

    def put_middle(j):
        @pl.when(j >= RING)
        def _():
            send_middle(j - RING).wait_send()

        def put(k, _):
            middle[j % RING, k] = near[table[per_zone + k]]
            return 0

        lax.fori_loop(0, cap, put, 0)
        send_middle(j).start()

    def finish(j):
        m, q, c = j // (parts * cuts), (j // cuts) % parts, j % cuts
        unit = pl.ds(pl.multiple_of(c * piece, piece), piece)
        lanes = lax.broadcasted_iota(jnp.int32, (piece, BLOCK), 1)

        def one(k, _):
            x = whole[table[3 * per_zone + k]].astype(jnp.float32)
            scale = jnp.max(jnp.abs(x), axis=2, keepdims=True) + EPS
            y = (x * (1.0 / scale)).astype(jnp.bfloat16)
            seen = jnp.where(q == 0, 0.0, kept[m, k, unit, :])
            for s in range(shards):
                start = pl.multiple_of(s * rows + q * BLOCK, BLOCK)
                out[m, k, unit, pl.ds(start, BLOCK)] = y[s]
                seen = jnp.where(lanes == s * parts + q, scale[s], seen)
            kept[m, k, unit, :] = seen
            return 0

        lax.fori_loop(0, per_zone, one, 0)

    for g in range(LOADS):
        start_load(jnp.int32(g))
    barrier = pltpu.get_barrier_semaphore()

    def greet(d, _):
        to = lax.rem(me + d, splits)
        pl.semaphore_signal(
            barrier, inc=1, device_id=(zone * 2 + to // shards, to % shards), device_id_type=MESH
        )
        return 0

    lax.fori_loop(1, splits, greet, 0)
    pl.semaphore_signal(barrier, inc=1, device_id=(neighbour, sub), device_id_type=MESH)

    @pl.when(is_inner)
    def _():
        pl.semaphore_signal(barrier, inc=1, device_id=(across, sub), device_id_type=MESH)

    turn(jnp.int32(0))
    pl.semaphore_wait(barrier, jnp.where(is_inner, splits + 1, splits))
    start_exchange(jnp.int32(0))
    for g in range(1, AHEAD):
        turn(jnp.int32(g))
        start_exchange(jnp.int32(g))

    def step(t, _):
        g = t // cuts + AHEAD

        @pl.when((t % cuts == 0) & (g < chunks))
        def _():
            @pl.when(g >= TURNS)
            def _():
                wait_turned(g % TURNS)

            turn(g)
            start_exchange(g)

        @pl.when(is_outer)
        def _():
            @pl.when(t < steps)
            def _():
                wait_exchange(t)
                gather(t, per_zone, near)
                put_beside(t, near)

            @pl.when(t >= LAG_OUT)
            def _():
                send_beside(t - LAG_OUT).wait_recv()
                gather(t - LAG_OUT, per_zone + edge, whole)
                finish(t - LAG_OUT)

        @pl.when(is_inner)
        def _():
            @pl.when(t < steps)
            def _():
                wait_exchange(t)
                send_beside(t).wait_recv()
                gather(t, per_zone + edge, near)
                put_middle(t)

            @pl.when((t >= LAG_IN) & (t < steps + LAG_IN))
            def _():
                send_middle(t - LAG_IN).wait_recv()
                gather(t - LAG_IN, 2 * per_zone + cap, whole)
                put_beside(t - LAG_IN, whole)
                finish(t - LAG_IN)

        return 0

    lax.fori_loop(0, steps + LAG_OUT, step, 0)
    for j in range(TURNS):
        wait_turned(j)
    for j in range(steps - RING, steps):
        send_beside(jnp.int32(j)).wait_send()

    @pl.when(is_inner)
    def _():
        for j in range(steps - RING, steps):
            send_middle(jnp.int32(j)).wait_send()


def tail_kernel(values, kept, packed, scales, sems):
    matrices, per_zone, columns, _ = values.shape

    def write(i):
        m, k = i // per_zone, i % per_zone
        return pltpu.make_async_copy(values.at[m, k], packed.at[m, k], sems.at[i])

    for i in range(matrices * per_zone):
        write(i).start()
    for m in range(matrices):
        for k in range(per_zone):
            scales[m, :, k * columns : (k + 1) * columns] = kept[m, k].T[: scales.shape[1], :]
    for i in range(matrices * per_zone):
        write(i).wait()


def line(cap, number, per_zone, shards, table, sources):
    local, rows, hidden = sources[0].shape
    columns = hidden // (2 * shards)
    matrices, full = len(sources), rows * shards
    blocks = full // BLOCK
    steps = matrices * (rows // BLOCK) * (columns // PIECE)
    edge = min(cap, per_zone)
    bf16, f32 = jnp.bfloat16, jnp.float32
    slot = (shards, PIECE, BLOCK)
    dma = pltpu.SemaphoreType.DMA
    slots = (steps + 1) * (2 * per_zone + cap) + 2 * per_zone + RING * (edge + cap)
    room = 2 * (slots * shards * PIECE * BLOCK + (LOADS + TURNS) * local * BLOCK * hidden)
    anywhere = pl.BlockSpec(memory_space=pl.ANY)
    vmem = pl.BlockSpec(memory_space=pltpu.VMEM)
    values, kept = pl.pallas_call(
        functools.partial(line_kernel, cap, per_zone),
        out_shape=(
            pltpu.VMEM((matrices, per_zone, columns, full), bf16),
            pltpu.VMEM((matrices, per_zone, columns, BLOCK), f32),
        ),
        in_specs=[pl.BlockSpec(memory_space=pltpu.SMEM)] + [anywhere] * matrices,
        out_specs=(vmem, vmem),
        scratch_shapes=[
            pltpu.VMEM((LOADS, local, BLOCK, hidden), bf16),
            pltpu.VMEM((TURNS, local, hidden, BLOCK), bf16),
            pltpu.VMEM((steps, 2 * per_zone + cap) + slot, bf16),
            pltpu.VMEM((RING, edge) + slot, bf16),
            pltpu.VMEM((RING, cap) + slot, bf16),
            pltpu.VMEM((2 * per_zone,) + slot, bf16),
            pltpu.VMEM((2 * per_zone + cap,) + slot, bf16),
            dma((LOADS,)),
            dma((TURNS,)),
            dma((steps,)),
            dma((RING,)),
            dma((steps,)),
            dma((RING,)),
            dma((steps,)),
        ],
        compiler_params=pltpu.CompilerParams(
            has_side_effects=True, collective_id=number, vmem_limit_bytes=room + 2**20
        ),
        name=f"line_{cap}",
    )(table, *sources)
    packed, scales = pl.pallas_call(
        tail_kernel,
        out_shape=(
            jax.ShapeDtypeStruct(values.shape, bf16),
            jax.ShapeDtypeStruct((matrices, blocks, per_zone * columns), f32),
        ),
        in_specs=[vmem, vmem],
        out_specs=(anywhere, vmem),
        scratch_shapes=[dma((matrices * per_zone,))],
        compiler_params=pltpu.CompilerParams(vmem_limit_bytes=2**22),
        name="tail",
    )(
        pltpu.with_memory_space_constraint(values, pltpu.VMEM),
        pltpu.with_memory_space_constraint(kept, pltpu.VMEM),
    )
    return (
        packed.reshape(matrices, 1, 1, per_zone, columns, full),
        scales.reshape(matrices, 1, 1, blocks, per_zone * columns),
    )


def per_device(gate_source, up_source, down_source, source_order, target_order):
    groups, shards = lax.axis_size("grp"), lax.axis_size("sub")
    sources = (gate_source, up_source, down_source)
    if groups != 8:
        return plain(*sources, source_order, target_order)
    per_zone = 2 * gate_source.shape[0]
    table, choice = plan(source_order, target_order, per_zone)

    def routed(cap, number):
        def run(table, sources):
            return line(cap, number, per_zone, shards, table, sources)

        return run

    branches = [routed(cap, i) for i, cap in enumerate(CAPS + (2 * per_zone,))]
    return lax.switch(choice[0], branches, table, sources)


def solution(mesh):
    placed = (P("grp", "sub", None), P("grp", "sub", None), P("grp", "sub", None), P(), P())
    return jax.shard_map(
        per_device,
        mesh=mesh,
        in_specs=placed,
        out_specs=(P(None, "grp", "sub", None, None, None), P(None, "grp", "sub", None, None)),
        check_vma=False,
    )
```

```python
import functools

import jax
import jax.numpy as jnp
from jax import lax
from jax.experimental import pallas as pl
from jax.experimental.pallas import tpu as pltpu
from jax.sharding import PartitionSpec as P

BLOCK = 128
EPS = 1e-06
MESH = pl.DeviceIdType.MESH
PIECE = 16
CASES = ((6, 6), (7, 6), (7, 7), (8, 7), (8, 8), (9, 8), (10, 8), (11, 8))
FIRST = 2
LAST = 1
LEAD = 3
HOLD = 16
LASTS = 20
LOADS = 3
TURNS = 4
RING = 6
TURN_AT = 3
LAG_IN = 2
LAG_OUT = 10


def pick(source_order, target_order):
    matches = source_order[None, :] == target_order[:, None]
    slots = jnp.arange(source_order.shape[0], dtype=jnp.int32)
    return jnp.sum(jnp.where(matches, slots[None, :], 0), axis=1, dtype=jnp.int32)


def plain(gate_source, up_source, down_source, source_order, target_order):
    stacked = jnp.stack([gate_source, up_source, down_source])
    matrices, local_slots, local_rows, hidden = stacked.shape
    groups = lax.axis_size("grp")
    shards = lax.axis_size("sub")
    devices = groups * shards
    experts = local_slots * groups
    full_rows = local_rows * shards
    targets = groups // 2
    per_group = experts // targets
    splits = 2 * shards
    columns = hidden // splits
    picked = pick(source_order, target_order)
    slab_rows = local_rows // devices
    pieces = stacked.reshape(matrices, 1, local_slots, devices, slab_rows, hidden)
    received = lax.all_to_all(pieces, ("grp", "sub"), split_axis=3, concat_axis=1, tiled=True)
    received = received.reshape(matrices, groups, shards, local_slots, slab_rows, hidden)
    received = received.transpose(0, 1, 3, 2, 4, 5).reshape(
        matrices, experts, shards * slab_rows, hidden
    )
    ordered = jnp.take(received, picked, axis=1)
    outgoing = ordered.reshape(matrices, targets, per_group, shards * slab_rows, splits, columns)
    outgoing = outgoing.transpose(0, 1, 4, 2, 3, 5).reshape(
        matrices, devices, per_group, 1, shards * slab_rows, columns
    )
    placed = lax.all_to_all(outgoing, ("grp", "sub"), split_axis=1, concat_axis=3, tiled=True)
    placed = placed.reshape(matrices, per_group, devices, shards, slab_rows, columns)
    placed = placed.transpose(0, 1, 3, 2, 4, 5).reshape(matrices, per_group, full_rows, columns)
    num_blocks = full_rows // BLOCK
    blocks = placed.astype(jnp.float32).reshape(matrices, per_group, num_blocks, BLOCK, columns)
    block_scale = jnp.max(jnp.abs(blocks), axis=3) + EPS
    quantized = (blocks / block_scale[:, :, :, None, :]).astype(jnp.bfloat16)
    quantized = quantized.reshape(matrices, per_group, full_rows, columns).transpose(0, 1, 3, 2)
    quantized = quantized.reshape(matrices, 1, 1, per_group, columns, full_rows)
    block_scale = block_scale.transpose(0, 2, 1, 3).reshape(
        matrices, 1, 1, num_blocks, per_group * columns
    )
    return (quantized, block_scale)


def plan_kernel(per_zone, source_order, target_order, table, choice, goes):
    experts = source_order.shape[0]
    spare = table.shape[0] - 1
    zone = lax.axis_index("grp") // 2
    i32 = jnp.int32

    def outer(z):
        return (z == 0) | (z == 3)

    def clear(i, _):
        table[i] = 0
        return 0

    lax.fori_loop(0, spare + 1, clear, 0, unroll=True)

    def note(j, _):
        goes[target_order[j]] = j
        return 0

    lax.fori_loop(0, experts, note, 0, unroll=True)

    def route(p, counts):
        in0, in3, out0, out3, first0, first1, last0, last1, rest0, rest1 = counts
        target = goes[source_order[p]]
        here, there, own = p // per_zone, target // per_zone, p % per_zone
        moves = here != there
        leaves = outer(here) & moves
        left = here < 2
        crosses = left != (there < 2)
        enters = outer(there) & moves
        rank_in = jnp.where(here == 0, in0, in3)
        rank_out = jnp.where(there == 0, out0, out3)
        first = jnp.where(left, first0, first1)
        final = jnp.where(left, last0, last1)
        rest = jnp.where(left, rest0, rest1)
        leads = crosses & jnp.logical_not(outer(here)) & (first < FIRST)
        trails = crosses & jnp.logical_not(leads) & jnp.logical_not(outer(there)) & (final < LAST)
        other = crosses & jnp.logical_not(leads | trails)
        seat = jnp.where(leads, first, jnp.where(trails, FIRST + final, FIRST + LAST + rest))
        on_inner = jnp.where(leaves, per_zone + rank_in, own)
        after_mid = jnp.where(crosses, 2 * per_zone + seat, on_inner)
        ends = jnp.where(moves, jnp.where(outer(there), per_zone + rank_out, after_mid), own)
        inward = leaves & (here == zone)
        table[jnp.where(inward, rank_in, spare)] = own
        outward = enters & jnp.logical_not(outer(zone)) & ((there < 2) == (zone < 2))
        table[jnp.where(outward, rank_out, spare)] = after_mid
        over = crosses & (left == (zone < 2))
        table[jnp.where(over, per_zone + seat, spare)] = on_inner
        stays = there == zone
        table[jnp.where(stays, 3 * per_zone + target % per_zone, spare)] = ends

        def add(flag):
            return jnp.where(flag, 1, 0).astype(i32)

        right = jnp.logical_not(left)
        return (
            in0 + add(leaves & (here == 0)),
            in3 + add(leaves & (here == 3)),
            out0 + add(enters & (there == 0)),
            out3 + add(enters & (there == 3)),
            first0 + add(leads & left),
            first1 + add(leads & right),
            last0 + add(trails & left),
            last1 + add(trails & right),
            rest0 + add(other & left),
            rest1 + add(other & right),
        )

    zero = jnp.zeros((), i32)
    counts = lax.fori_loop(0, experts, route, (zero,) * 10, unroll=True)
    beside = jnp.maximum(counts[0], counts[1])
    middle = FIRST + LAST + jnp.maximum(counts[8], counts[9])
    index = jnp.full((), len(CASES), i32)
    for i in range(len(CASES) - 1, -1, -1):
        cap, edge = CASES[i]
        index = jnp.where((middle <= cap) & (beside <= edge), i, index)
    choice[0] = index


def plan(source_order, target_order, per_zone):
    smem = pl.BlockSpec(memory_space=pltpu.SMEM)
    return pl.pallas_call(
        functools.partial(plan_kernel, per_zone),
        out_shape=(
            jax.ShapeDtypeStruct((4 * per_zone + 1,), jnp.int32),
            jax.ShapeDtypeStruct((1,), jnp.int32),
        ),
        in_specs=[smem, smem],
        out_specs=(smem, smem),
        scratch_shapes=[pltpu.SMEM(source_order.shape, jnp.int32)],
        name="plan",
    )(source_order, target_order)


def line_kernel(cap, per_zone, table, *refs):
    sources, out, kept = refs[:3], refs[3], refs[4]
    raw, turned, held, beside, lead, middle, last, near, whole = refs[5:14]
    in_sem, ex_send, ex_recv, be_send, be_recv = refs[14:19]
    le_send, le_recv, mi_send, mi_recv, la_send, la_recv = refs[19:]
    grp, sub = lax.axis_index("grp"), lax.axis_index("sub")
    zone, half = grp // 2, grp % 2
    matrices = len(sources)
    local, rows, hidden = sources[0].shape
    steps, _, shards, piece, _ = held.shape
    edge = beside.shape[1]
    splits = 2 * shards
    columns = hidden // splits
    cuts = columns // piece
    parts = rows // BLOCK
    chunks = matrices * parts
    me = half * shards + sub
    is_outer = (zone == 0) | (zone == 3)
    is_inner = (zone == 1) | (zone == 2)
    neighbour = (zone + 1 - 2 * (zone % 2)) * 2 + half
    across = (3 - zone) * 2 + half

    def load(g, i):
        return pltpu.make_async_copy(
            sources[i].at[:, pl.ds(pl.multiple_of((g % parts) * BLOCK, BLOCK), BLOCK), :],
            raw.at[g % LOADS],
            in_sem.at[g % LOADS],
        )

    def start_load(g):
        for i in range(matrices):

            @pl.when(g // parts == i)
            def _():
                load(g, i).start()

    def exchange(g, c, to):
        start = pl.multiple_of(to * columns + c * piece, 16)
        return pltpu.make_async_remote_copy(
            src_ref=turned.at[g % TURNS, :, pl.ds(start, piece), :],
            dst_ref=held.at[g * cuts + c, pl.ds(half * local, local), sub],
            send_sem=ex_send.at[g % TURNS],
            recv_sem=ex_recv.at[g * cuts + c],
            device_id=(zone * 2 + to // shards, to % shards),
            device_id_type=MESH,
        )

    def turn(g):
        load(g, 0).wait()

        def one(e, _):
            for b in range(hidden // BLOCK):
                turned[g % TURNS, e, b * BLOCK : (b + 1) * BLOCK, :] = raw[
                    g % LOADS, e, :, b * BLOCK : (b + 1) * BLOCK
                ].T
            return 0

        lax.fori_loop(0, local, one, 0, unroll=True)

        @pl.when(g + LOADS < chunks)
        def _():
            start_load(g + LOADS)

    def start_exchange(g):
        def cut(c, _):
            start = pl.multiple_of(me * columns + c * piece, 16)
            pltpu.make_async_copy(
                turned.at[g % TURNS, :, pl.ds(start, piece), :],
                held.at[g * cuts + c, pl.ds(half * local, local), sub],
                ex_recv.at[g * cuts + c],
            ).start()

            def go(d, _):
                exchange(g, c, lax.rem(me + d, splits)).start()
                return 0

            return lax.fori_loop(1, splits, go, 0)

        lax.fori_loop(0, cuts, cut, 0)

    def wait_exchange(j):
        mine = held.at[j, pl.ds(0, per_zone)]
        pltpu.make_async_copy(mine, mine, ex_recv.at[j]).wait()

    def gather(j, work, *ranges):
        for slots in ranges:
            for i in slots:
                work[i] = held[j, i]

    def wait_turned(slot):
        sent = turned.at[slot, :, pl.ds(0, (splits - 1) * columns), :]
        pltpu.make_async_copy(sent, sent, ex_send.at[slot]).wait()

    def send_beside(j):
        return pltpu.make_async_remote_copy(
            src_ref=beside.at[j % RING], dst_ref=held.at[j, pl.ds(per_zone, edge)],
            send_sem=be_send.at[j % RING], recv_sem=be_recv.at[j],
            device_id=(neighbour, sub), device_id_type=MESH,
        )

    at_lead = 2 * per_zone
    at_last = at_lead + FIRST
    at_rest = at_last + LAST

    def send_across(j, ref, depth, start, send_sem, recv_sem):
        return pltpu.make_async_remote_copy(
            src_ref=ref.at[j % depth], dst_ref=held.at[j, pl.ds(start, ref.shape[1])],
            send_sem=send_sem.at[j % depth], recv_sem=recv_sem.at[j],
            device_id=(across, sub), device_id_type=MESH,
        )

    def send_lead(j):
        return send_across(j, lead, RING, at_lead, le_send, le_recv)

    def send_middle(j):
        return send_across(j, middle, RING, at_rest, mi_send, mi_recv)

    def send_last(j):
        return send_across(j, last, LASTS, at_last, la_send, la_recv)

    def put_beside(j, work):
        @pl.when(j >= RING)
        def _():
            send_beside(j - RING).wait_send()

        def put(k, _):
            beside[j % RING, k] = work[table[k]]
            return 0

        lax.fori_loop(0, edge, put, 0, unroll=True)
        send_beside(j).start()

    def put_across(j, ref, depth, send, start):
        @pl.when(j >= depth)
        def _():
            send(j - depth).wait_send()

        for k in range(ref.shape[1]):
            ref[j % depth, k] = near[table[per_zone + start - at_lead + k]]

    def finish(j):
        m, q, c = j // (parts * cuts), (j // cuts) % parts, j % cuts
        unit = pl.ds(pl.multiple_of(c * piece, piece), piece)
        lanes = lax.broadcasted_iota(jnp.int32, (piece, BLOCK), 1)

        def one(k, _):
            x = whole[table[3 * per_zone + k]].astype(jnp.float32)
            scale = jnp.max(jnp.abs(x), axis=2, keepdims=True) + EPS
            y = (x * (1.0 / scale)).astype(jnp.bfloat16)
            seen = jnp.where(q == 0, 0.0, kept[m, k, unit, :])
            for s in range(shards):
                start = pl.multiple_of(s * rows + q * BLOCK, BLOCK)
                out[m, k, unit, pl.ds(start, BLOCK)] = y[s]
                seen = jnp.where(lanes == s * parts + q, scale[s], seen)
            kept[m, k, unit, :] = seen
            return 0

        lax.fori_loop(0, per_zone, one, 0, unroll=True)

    for g in range(LOADS):
        start_load(jnp.int32(g))
    barrier = pltpu.get_barrier_semaphore()

    def greet(d, _):
        to = lax.rem(me + d, splits)
        pl.semaphore_signal(
            barrier, inc=1, device_id=(zone * 2 + to // shards, to % shards), device_id_type=MESH
        )
        return 0

    lax.fori_loop(1, splits, greet, 0)
    pl.semaphore_signal(barrier, inc=1, device_id=(neighbour, sub), device_id_type=MESH)

    @pl.when(is_inner)
    def _():
        pl.semaphore_signal(barrier, inc=1, device_id=(across, sub), device_id_type=MESH)

    turn(jnp.int32(0))
    pl.semaphore_wait(barrier, jnp.where(is_inner, splits + 1, splits))
    start_exchange(jnp.int32(0))

    mine, both = range(per_zone), range(per_zone + edge)

    def step(u, _):
        @pl.when(is_outer)
        def _():
            @pl.when(u < steps)
            def _():
                wait_exchange(u)
                gather(u, near, mine)
                put_beside(u, near)

            f = u - LAG_OUT

            @pl.when((f >= 0) & (f < steps))
            def _():
                send_beside(f).wait_recv()
                gather(f, whole, both)
                finish(f)

        @pl.when(is_inner)
        def _():
            @pl.when(u < steps)
            def _():
                wait_exchange(u)
                gather(u, near, mine)
                put_across(u, lead, RING, send_lead, at_lead)
                send_lead(u).start()

            t = u - LEAD

            @pl.when((t >= 0) & (t < steps))
            def _():
                send_beside(t).wait_recv()
                gather(t, near, both)
                put_across(t, middle, RING, send_middle, at_rest)
                send_middle(t).start()
                put_across(t, last, LASTS, send_last, at_last)

                @pl.when(t >= HOLD)
                def _():
                    send_last(t - HOLD).start()

                @pl.when(t == steps - 1)
                def _():
                    def go(j, _):
                        send_last(j).start()
                        return 0

                    lax.fori_loop(steps - HOLD, steps, go, 0)

            i = t - LAG_IN

            @pl.when((i >= 0) & (i < steps))
            def _():
                send_lead(i).wait_recv()
                send_middle(i).wait_recv()
                gather(i, whole, both, range(at_lead, at_last), range(at_rest, at_lead + cap))
                put_beside(i, whole)

            f = i - HOLD

            @pl.when((f >= 0) & (f < steps))
            def _():
                send_last(f).wait_recv()
                gather(f, whole, both, range(at_lead, at_lead + cap))
                finish(f)

        g = u // cuts + 1

        @pl.when((u % cuts == TURN_AT) & (g < chunks))
        def _():
            @pl.when(g >= TURNS)
            def _():
                wait_turned(g % TURNS)

            turn(g)
            start_exchange(g)

        return 0

    lax.fori_loop(0, steps + max(LAG_OUT, LEAD + LAG_IN + HOLD), step, 0)
    for j in range(TURNS):
        wait_turned(j)
    for j in range(steps - RING, steps):
        send_beside(jnp.int32(j)).wait_send()

    @pl.when(is_inner)
    def _():
        for j in range(steps - RING, steps):
            send_lead(jnp.int32(j)).wait_send()
            send_middle(jnp.int32(j)).wait_send()
        for j in range(steps - LASTS, steps):
            send_last(jnp.int32(j)).wait_send()


def tail_kernel(values, kept, packed, scales, ready, sems, sem):
    matrices, per_zone, columns, _ = values.shape

    def write(i):
        m, k = i // per_zone, i % per_zone
        return pltpu.make_async_copy(values.at[m, k], packed.at[m, k], sems.at[i])

    for i in range(matrices * per_zone):
        write(i).start()
    for m in range(matrices):
        for k in range(per_zone):
            ready[m, :, k * columns : (k + 1) * columns] = kept[m, k].T[: ready.shape[1], :]
    last = pltpu.make_async_copy(ready, scales, sem)
    last.start()
    for i in range(matrices * per_zone):
        write(i).wait()
    last.wait()


def line(cap, edge, number, per_zone, shards, table, sources):
    local, rows, hidden = sources[0].shape
    columns = hidden // (2 * shards)
    matrices, full = len(sources), rows * shards
    blocks = full // BLOCK
    steps = matrices * (rows // BLOCK) * (columns // PIECE)
    rest = cap - FIRST - LAST
    bf16, f32 = jnp.bfloat16, jnp.float32
    slot = (shards, PIECE, BLOCK)
    dma = pltpu.SemaphoreType.DMA
    slots = (steps + 1) * (2 * per_zone + cap) + 2 * per_zone
    slots += RING * (edge + FIRST + rest) + LASTS * LAST
    room = 2 * (slots * shards * PIECE * BLOCK + (LOADS + TURNS) * local * BLOCK * hidden)
    anywhere = pl.BlockSpec(memory_space=pl.ANY)
    vmem = pl.BlockSpec(memory_space=pltpu.VMEM)
    values, kept = pl.pallas_call(
        functools.partial(line_kernel, cap, per_zone),
        out_shape=(
            pltpu.VMEM((matrices, per_zone, columns, full), bf16),
            pltpu.VMEM((matrices, per_zone, columns, BLOCK), f32),
        ),
        in_specs=[pl.BlockSpec(memory_space=pltpu.SMEM)] + [anywhere] * matrices,
        out_specs=(vmem, vmem),
        scratch_shapes=[
            pltpu.VMEM((LOADS, local, BLOCK, hidden), bf16),
            pltpu.VMEM((TURNS, local, hidden, BLOCK), bf16),
            pltpu.VMEM((steps, 2 * per_zone + cap) + slot, bf16),
            pltpu.VMEM((RING, edge) + slot, bf16),
            pltpu.VMEM((RING, FIRST) + slot, bf16),
            pltpu.VMEM((RING, rest) + slot, bf16),
            pltpu.VMEM((LASTS, LAST) + slot, bf16),
            pltpu.VMEM((2 * per_zone,) + slot, bf16),
            pltpu.VMEM((2 * per_zone + cap,) + slot, bf16),
            dma((LOADS,)),
            dma((TURNS,)),
            dma((steps,)),
            dma((RING,)),
            dma((steps,)),
            dma((RING,)),
            dma((steps,)),
            dma((RING,)),
            dma((steps,)),
            dma((LASTS,)),
            dma((steps,)),
        ],
        compiler_params=pltpu.CompilerParams(
            has_side_effects=True, collective_id=number, vmem_limit_bytes=room + 2**20
        ),
        name=f"line_{cap}_{edge}",
    )(table, *sources)
    packed, scales = pl.pallas_call(
        tail_kernel,
        out_shape=(
            jax.ShapeDtypeStruct(values.shape, bf16),
            jax.ShapeDtypeStruct((matrices, blocks, per_zone * columns), f32),
        ),
        in_specs=[vmem, vmem],
        out_specs=(anywhere, anywhere),
        scratch_shapes=[
            pltpu.VMEM((matrices, blocks, per_zone * columns), f32),
            dma((matrices * per_zone,)),
            dma(()),
        ],
        compiler_params=pltpu.CompilerParams(vmem_limit_bytes=2**22),
        name="tail",
    )(
        pltpu.with_memory_space_constraint(values, pltpu.VMEM),
        pltpu.with_memory_space_constraint(kept, pltpu.VMEM),
    )
    return (
        packed.reshape(matrices, 1, 1, per_zone, columns, full),
        scales.reshape(matrices, 1, 1, blocks, per_zone * columns),
    )


def per_device(gate_source, up_source, down_source, source_order, target_order):
    groups, shards = lax.axis_size("grp"), lax.axis_size("sub")
    sources = (gate_source, up_source, down_source)
    if groups != 8:
        return plain(*sources, source_order, target_order)
    per_zone = 2 * gate_source.shape[0]
    table, choice = plan(source_order, target_order, per_zone)

    def routed(number, cap, edge):
        def run(table, sources):
            return line(cap, edge, number, per_zone, shards, table, sources)

        return run

    cases = CASES + ((2 * per_zone, per_zone),)
    branches = [routed(i, *case) for i, case in enumerate(cases)]
    return lax.switch(choice[0], branches, table, sources)


def solution(mesh):
    placed = (P("grp", "sub", None), P("grp", "sub", None), P("grp", "sub", None), P(), P())
    return jax.shard_map(
        per_device,
        mesh=mesh,
        in_specs=placed,
        out_specs=(P(None, "grp", "sub", None, None, None), P(None, "grp", "sub", None, None)),
        check_vma=False,
    )
```

```python
import functools

import jax
import jax.numpy as jnp
from jax import lax
from jax.experimental import pallas as pl
from jax.experimental.pallas import tpu as pltpu
from jax.sharding import PartitionSpec as P

BLOCK = 128
EPS = 1e-06
MESH = pl.DeviceIdType.MESH
PIECE = 16
CASES = ((6, 6), (7, 6), (7, 7), (8, 7), (8, 8), (9, 8), (10, 8), (11, 8))
FIRST = 2
LAST = 1
LEAD = 3
HOLD = 16
LASTS = 20
ARRIVE = 12
LOADS = 3
TURNS = 4
RING = 6
TURN_AT = 3
LAG_IN = 2
LAG_OUT = 10


def pick(source_order, target_order):
    matches = source_order[None, :] == target_order[:, None]
    slots = jnp.arange(source_order.shape[0], dtype=jnp.int32)
    return jnp.sum(jnp.where(matches, slots[None, :], 0), axis=1, dtype=jnp.int32)


def plain(gate_source, up_source, down_source, source_order, target_order):
    stacked = jnp.stack([gate_source, up_source, down_source])
    matrices, local_slots, local_rows, hidden = stacked.shape
    groups = lax.axis_size("grp")
    shards = lax.axis_size("sub")
    devices = groups * shards
    experts = local_slots * groups
    full_rows = local_rows * shards
    targets = groups // 2
    per_group = experts // targets
    splits = 2 * shards
    columns = hidden // splits
    picked = pick(source_order, target_order)
    slab_rows = local_rows // devices
    pieces = stacked.reshape(matrices, 1, local_slots, devices, slab_rows, hidden)
    received = lax.all_to_all(pieces, ("grp", "sub"), split_axis=3, concat_axis=1, tiled=True)
    received = received.reshape(matrices, groups, shards, local_slots, slab_rows, hidden)
    received = received.transpose(0, 1, 3, 2, 4, 5).reshape(
        matrices, experts, shards * slab_rows, hidden
    )
    ordered = jnp.take(received, picked, axis=1)
    outgoing = ordered.reshape(matrices, targets, per_group, shards * slab_rows, splits, columns)
    outgoing = outgoing.transpose(0, 1, 4, 2, 3, 5).reshape(
        matrices, devices, per_group, 1, shards * slab_rows, columns
    )
    placed = lax.all_to_all(outgoing, ("grp", "sub"), split_axis=1, concat_axis=3, tiled=True)
    placed = placed.reshape(matrices, per_group, devices, shards, slab_rows, columns)
    placed = placed.transpose(0, 1, 3, 2, 4, 5).reshape(matrices, per_group, full_rows, columns)
    num_blocks = full_rows // BLOCK
    blocks = placed.astype(jnp.float32).reshape(matrices, per_group, num_blocks, BLOCK, columns)
    block_scale = jnp.max(jnp.abs(blocks), axis=3) + EPS
    quantized = (blocks / block_scale[:, :, :, None, :]).astype(jnp.bfloat16)
    quantized = quantized.reshape(matrices, per_group, full_rows, columns).transpose(0, 1, 3, 2)
    quantized = quantized.reshape(matrices, 1, 1, per_group, columns, full_rows)
    block_scale = block_scale.transpose(0, 2, 1, 3).reshape(
        matrices, 1, 1, num_blocks, per_group * columns
    )
    return (quantized, block_scale)


def plan_kernel(per_zone, source_order, target_order, table, choice, goes):
    experts = source_order.shape[0]
    spare = table.shape[0] - 1
    zone = lax.axis_index("grp") // 2
    i32 = jnp.int32

    def outer(z):
        return (z == 0) | (z == 3)

    def clear(i, _):
        table[i] = 0
        return 0

    lax.fori_loop(0, spare + 1, clear, 0, unroll=True)

    def note(j, _):
        goes[target_order[j]] = j
        return 0

    lax.fori_loop(0, experts, note, 0, unroll=True)

    def route(p, counts):
        in0, in3, out0, out3, first0, first1, last0, last1, rest0, rest1 = counts
        target = goes[source_order[p]]
        here, there, own = p // per_zone, target // per_zone, p % per_zone
        moves = here != there
        leaves = outer(here) & moves
        left = here < 2
        crosses = left != (there < 2)
        enters = outer(there) & moves
        rank_in = jnp.where(here == 0, in0, in3)
        rank_out = jnp.where(there == 0, out0, out3)
        first = jnp.where(left, first0, first1)
        final = jnp.where(left, last0, last1)
        rest = jnp.where(left, rest0, rest1)
        leads = crosses & jnp.logical_not(outer(here)) & (first < FIRST)
        trails = crosses & jnp.logical_not(leads) & jnp.logical_not(outer(there)) & (final < LAST)
        other = crosses & jnp.logical_not(leads | trails)
        seat = jnp.where(leads, first, jnp.where(trails, FIRST + final, FIRST + LAST + rest))
        on_inner = jnp.where(leaves, per_zone + rank_in, own)
        after_mid = jnp.where(crosses, 2 * per_zone + seat, on_inner)
        ends = jnp.where(moves, jnp.where(outer(there), per_zone + rank_out, after_mid), own)
        inward = leaves & (here == zone)
        table[jnp.where(inward, rank_in, spare)] = own
        outward = enters & jnp.logical_not(outer(zone)) & ((there < 2) == (zone < 2))
        table[jnp.where(outward, rank_out, spare)] = after_mid
        over = crosses & (left == (zone < 2))
        table[jnp.where(over, per_zone + seat, spare)] = on_inner
        stays = there == zone
        table[jnp.where(stays, 3 * per_zone + target % per_zone, spare)] = ends

        def add(flag):
            return jnp.where(flag, 1, 0).astype(i32)

        right = jnp.logical_not(left)
        return (
            in0 + add(leaves & (here == 0)),
            in3 + add(leaves & (here == 3)),
            out0 + add(enters & (there == 0)),
            out3 + add(enters & (there == 3)),
            first0 + add(leads & left),
            first1 + add(leads & right),
            last0 + add(trails & left),
            last1 + add(trails & right),
            rest0 + add(other & left),
            rest1 + add(other & right),
        )

    zero = jnp.zeros((), i32)
    counts = lax.fori_loop(0, experts, route, (zero,) * 10, unroll=True)
    beside = jnp.maximum(counts[0], counts[1])
    middle = FIRST + LAST + jnp.maximum(counts[8], counts[9])
    index = jnp.full((), len(CASES), i32)
    for i in range(len(CASES) - 1, -1, -1):
        cap, edge = CASES[i]
        index = jnp.where((middle <= cap) & (beside <= edge), i, index)
    choice[0] = index


def plan(source_order, target_order, per_zone):
    smem = pl.BlockSpec(memory_space=pltpu.SMEM)
    return pl.pallas_call(
        functools.partial(plan_kernel, per_zone),
        out_shape=(
            jax.ShapeDtypeStruct((4 * per_zone + 1,), jnp.int32),
            jax.ShapeDtypeStruct((1,), jnp.int32),
        ),
        in_specs=[smem, smem],
        out_specs=(smem, smem),
        scratch_shapes=[pltpu.SMEM(source_order.shape, jnp.int32)],
        name="plan",
    )(source_order, target_order)


def line_kernel(cap, per_zone, table, *refs):
    sources, out, kept = refs[:3], refs[3], refs[4]
    raw, turned, held, beside, lead, middle, last, near, whole = refs[5:14]
    in_sem, ex_send, ex_recv, be_send, be_recv = refs[14:19]
    le_send, le_recv, mi_send, mi_recv, la_send, la_recv = refs[19:]
    grp, sub = lax.axis_index("grp"), lax.axis_index("sub")
    zone, half = grp // 2, grp % 2
    matrices = len(sources)
    local, rows, hidden = sources[0].shape
    steps, _, shards, piece, _ = held.shape
    edge = beside.shape[1]
    splits = 2 * shards
    columns = hidden // splits
    cuts = columns // piece
    parts = rows // BLOCK
    chunks = matrices * parts
    exchanges = ex_recv.shape[0]
    me = half * shards + sub
    is_outer = (zone == 0) | (zone == 3)
    is_inner = (zone == 1) | (zone == 2)
    neighbour = (zone + 1 - 2 * (zone % 2)) * 2 + half
    across = (3 - zone) * 2 + half

    def load(g, i):
        return pltpu.make_async_copy(
            sources[i].at[:, pl.ds(pl.multiple_of((g % parts) * BLOCK, BLOCK), BLOCK), :],
            raw.at[g % LOADS],
            in_sem.at[g % LOADS],
        )

    def start_load(g):
        for i in range(matrices):

            @pl.when(g // parts == i)
            def _():
                load(g, i).start()

    def exchange(g, c, to):
        start = pl.multiple_of(to * columns + c * piece, 16)
        return pltpu.make_async_remote_copy(
            src_ref=turned.at[g % TURNS, :, pl.ds(start, piece), :],
            dst_ref=held.at[g * cuts + c, pl.ds(half * local, local), sub],
            send_sem=ex_send.at[g % TURNS],
            recv_sem=ex_recv.at[(g * cuts + c) % exchanges],
            device_id=(zone * 2 + to // shards, to % shards),
            device_id_type=MESH,
        )

    def turn(g):
        load(g, 0).wait()

        def one(e, _):
            for b in range(hidden // BLOCK):
                turned[g % TURNS, e, b * BLOCK : (b + 1) * BLOCK, :] = raw[
                    g % LOADS, e, :, b * BLOCK : (b + 1) * BLOCK
                ].T
            return 0

        lax.fori_loop(0, local, one, 0, unroll=True)

        @pl.when(g + LOADS < chunks)
        def _():
            start_load(g + LOADS)

    def start_exchange(g):
        def cut(c, _):
            start = pl.multiple_of(me * columns + c * piece, 16)
            pltpu.make_async_copy(
                turned.at[g % TURNS, :, pl.ds(start, piece), :],
                held.at[g * cuts + c, pl.ds(half * local, local), sub],
                ex_recv.at[(g * cuts + c) % exchanges],
            ).start()

            def go(d, _):
                exchange(g, c, lax.rem(me + d, splits)).start()
                return 0

            return lax.fori_loop(1, splits, go, 0)

        lax.fori_loop(0, cuts, cut, 0)

    def wait_exchange(j):
        mine = held.at[j, pl.ds(0, per_zone)]
        pltpu.make_async_copy(mine, mine, ex_recv.at[j % exchanges]).wait()

    def gather(j, work, *ranges):
        for slots in ranges:
            for i in slots:
                work[i] = held[j, i]

    def wait_turned(slot):
        sent = turned.at[slot, :, pl.ds(0, (splits - 1) * columns), :]
        pltpu.make_async_copy(sent, sent, ex_send.at[slot]).wait()

    def send_beside(j):
        return pltpu.make_async_remote_copy(
            src_ref=beside.at[j % RING], dst_ref=held.at[j, pl.ds(per_zone, edge)],
            send_sem=be_send.at[j % RING], recv_sem=be_recv.at[j % ARRIVE],
            device_id=(neighbour, sub), device_id_type=MESH,
        )

    at_lead = 2 * per_zone
    at_last = at_lead + FIRST
    at_rest = at_last + LAST

    def send_across(j, ref, depth, start, send_sem, recv_sem):
        return pltpu.make_async_remote_copy(
            src_ref=ref.at[j % depth], dst_ref=held.at[j, pl.ds(start, ref.shape[1])],
            send_sem=send_sem.at[j % depth], recv_sem=recv_sem.at[j % recv_sem.shape[0]],
            device_id=(across, sub), device_id_type=MESH,
        )

    def send_lead(j):
        return send_across(j, lead, RING, at_lead, le_send, le_recv)

    def send_middle(j):
        return send_across(j, middle, RING, at_rest, mi_send, mi_recv)

    def send_last(j):
        return send_across(j, last, LASTS, at_last, la_send, la_recv)

    def put_beside(j, work):
        @pl.when(j >= RING)
        def _():
            send_beside(j - RING).wait_send()

        def put(k, _):
            beside[j % RING, k] = work[table[k]]
            return 0

        lax.fori_loop(0, edge, put, 0, unroll=True)
        send_beside(j).start()

    def put_across(j, ref, depth, send, start):
        @pl.when(j >= depth)
        def _():
            send(j - depth).wait_send()

        for k in range(ref.shape[1]):
            ref[j % depth, k] = near[table[per_zone + start - at_lead + k]]

    def finish(j):
        m, q, c = j // (parts * cuts), (j // cuts) % parts, j % cuts
        unit = pl.ds(pl.multiple_of(c * piece, piece), piece)
        lanes = lax.broadcasted_iota(jnp.int32, (piece, BLOCK), 1)

        def one(k, _):
            x = whole[table[3 * per_zone + k]].astype(jnp.float32)
            scale = jnp.max(jnp.abs(x), axis=2, keepdims=True) + EPS
            y = (x * (1.0 / scale)).astype(jnp.bfloat16)
            seen = jnp.where(q == 0, 0.0, kept[m, k, unit, :])
            for s in range(shards):
                start = pl.multiple_of(s * rows + q * BLOCK, BLOCK)
                out[m, k, unit, pl.ds(start, BLOCK)] = y[s]
                seen = jnp.where(lanes == s * parts + q, scale[s], seen)
            kept[m, k, unit, :] = seen
            return 0

        lax.fori_loop(0, per_zone, one, 0, unroll=True)

    for g in range(LOADS):
        start_load(jnp.int32(g))
    barrier = pltpu.get_barrier_semaphore()

    def greet(d, _):
        to = lax.rem(me + d, splits)
        pl.semaphore_signal(
            barrier, inc=1, device_id=(zone * 2 + to // shards, to % shards), device_id_type=MESH
        )
        return 0

    lax.fori_loop(1, splits, greet, 0)
    pl.semaphore_signal(barrier, inc=1, device_id=(neighbour, sub), device_id_type=MESH)

    @pl.when(is_inner)
    def _():
        pl.semaphore_signal(barrier, inc=1, device_id=(across, sub), device_id_type=MESH)

    turn(jnp.int32(0))
    pl.semaphore_wait(barrier, jnp.where(is_inner, splits + 1, splits))
    start_exchange(jnp.int32(0))

    mine, both = range(per_zone), range(per_zone + edge)

    def step(u, _):
        @pl.when(is_outer)
        def _():
            @pl.when(u < steps)
            def _():
                wait_exchange(u)
                gather(u, near, mine)
                put_beside(u, near)

            f = u - LAG_OUT

            @pl.when((f >= 0) & (f < steps))
            def _():
                send_beside(f).wait_recv()
                gather(f, whole, both)
                finish(f)

        @pl.when(is_inner)
        def _():
            @pl.when(u < steps)
            def _():
                wait_exchange(u)
                gather(u, near, mine)
                put_across(u, lead, RING, send_lead, at_lead)
                send_lead(u).start()

            t = u - LEAD

            @pl.when((t >= 0) & (t < steps))
            def _():
                send_beside(t).wait_recv()
                gather(t, near, both)
                put_across(t, middle, RING, send_middle, at_rest)
                send_middle(t).start()
                put_across(t, last, LASTS, send_last, at_last)

                @pl.when(t >= HOLD)
                def _():
                    send_last(t - HOLD).start()

                @pl.when(t == steps - 1)
                def _():
                    def go(j, _):
                        send_last(j).start()
                        return 0

                    lax.fori_loop(steps - HOLD, steps, go, 0)

            i = t - LAG_IN

            @pl.when((i >= 0) & (i < steps))
            def _():
                send_lead(i).wait_recv()
                send_middle(i).wait_recv()
                gather(i, whole, both, range(at_lead, at_last), range(at_rest, at_lead + cap))
                put_beside(i, whole)

            f = i - HOLD

            @pl.when((f >= 0) & (f < steps))
            def _():
                send_last(f).wait_recv()
                gather(f, whole, both, range(at_lead, at_lead + cap))
                finish(f)

        g = u // cuts + 1

        @pl.when((u % cuts == TURN_AT) & (g < chunks))
        def _():
            @pl.when(g >= TURNS)
            def _():
                wait_turned(g % TURNS)

            turn(g)
            start_exchange(g)

        return 0

    lax.fori_loop(0, steps + max(LAG_OUT, LEAD + LAG_IN + HOLD), step, 0)
    for j in range(TURNS):
        wait_turned(j)
    for j in range(steps - RING, steps):
        send_beside(jnp.int32(j)).wait_send()

    @pl.when(is_inner)
    def _():
        for j in range(steps - RING, steps):
            send_lead(jnp.int32(j)).wait_send()
            send_middle(jnp.int32(j)).wait_send()
        for j in range(steps - LASTS, steps):
            send_last(jnp.int32(j)).wait_send()


def tail_kernel(values, kept, packed, scales, ready, sems, sem):
    matrices, per_zone, columns, _ = values.shape

    def write(i):
        m, k = i // per_zone, i % per_zone
        return pltpu.make_async_copy(values.at[m, k], packed.at[m, k], sems.at[0])

    for i in range(matrices * per_zone):
        write(i).start()
    for m in range(matrices):
        for k in range(per_zone):
            ready[m, :, k * columns : (k + 1) * columns] = kept[m, k].T[: ready.shape[1], :]
    last = pltpu.make_async_copy(ready, scales, sem)
    last.start()
    pltpu.make_async_copy(values, packed, sems.at[0]).wait()
    last.wait()


def line(cap, edge, number, per_zone, shards, table, sources):
    local, rows, hidden = sources[0].shape
    columns = hidden // (2 * shards)
    matrices, full = len(sources), rows * shards
    blocks = full // BLOCK
    steps = matrices * (rows // BLOCK) * (columns // PIECE)
    rest = cap - FIRST - LAST
    bf16, f32 = jnp.bfloat16, jnp.float32
    slot = (shards, PIECE, BLOCK)
    dma = pltpu.SemaphoreType.DMA
    slots = (steps + 1) * (2 * per_zone + cap) + 2 * per_zone
    slots += RING * (edge + FIRST + rest) + LASTS * LAST
    room = 2 * (slots * shards * PIECE * BLOCK + (LOADS + TURNS) * local * BLOCK * hidden)
    anywhere = pl.BlockSpec(memory_space=pl.ANY)
    vmem = pl.BlockSpec(memory_space=pltpu.VMEM)
    values, kept = pl.pallas_call(
        functools.partial(line_kernel, cap, per_zone),
        out_shape=(
            pltpu.VMEM((matrices, per_zone, columns, full), bf16),
            pltpu.VMEM((matrices, per_zone, columns, BLOCK), f32),
        ),
        in_specs=[pl.BlockSpec(memory_space=pltpu.SMEM)] + [anywhere] * matrices,
        out_specs=(vmem, vmem),
        scratch_shapes=[
            pltpu.VMEM((LOADS, local, BLOCK, hidden), bf16),
            pltpu.VMEM((TURNS, local, hidden, BLOCK), bf16),
            pltpu.VMEM((steps, 2 * per_zone + cap) + slot, bf16),
            pltpu.VMEM((RING, edge) + slot, bf16),
            pltpu.VMEM((RING, FIRST) + slot, bf16),
            pltpu.VMEM((RING, rest) + slot, bf16),
            pltpu.VMEM((LASTS, LAST) + slot, bf16),
            pltpu.VMEM((2 * per_zone,) + slot, bf16),
            pltpu.VMEM((2 * per_zone + cap,) + slot, bf16),
            dma((LOADS,)),
            dma((TURNS,)),
            dma((3 * columns // PIECE,)),
            dma((RING,)),
            dma((ARRIVE,)),
            dma((RING,)),
            dma((ARRIVE,)),
            dma((RING,)),
            dma((ARRIVE,)),
            dma((LASTS,)),
            dma((HOLD + 8,)),
        ],
        compiler_params=pltpu.CompilerParams(
            has_side_effects=True, collective_id=number, vmem_limit_bytes=room + 2**20
        ),
        name=f"line_{cap}_{edge}",
    )(table, *sources)
    packed, scales = pl.pallas_call(
        tail_kernel,
        out_shape=(
            jax.ShapeDtypeStruct(values.shape, bf16),
            jax.ShapeDtypeStruct((matrices, blocks, per_zone * columns), f32),
        ),
        in_specs=[vmem, vmem],
        out_specs=(anywhere, anywhere),
        scratch_shapes=[
            pltpu.VMEM((matrices, blocks, per_zone * columns), f32),
            dma((1,)),
            dma(()),
        ],
        compiler_params=pltpu.CompilerParams(vmem_limit_bytes=2**22),
        name="tail",
    )(
        pltpu.with_memory_space_constraint(values, pltpu.VMEM),
        pltpu.with_memory_space_constraint(kept, pltpu.VMEM),
    )
    return (
        packed.reshape(matrices, 1, 1, per_zone, columns, full),
        scales.reshape(matrices, 1, 1, blocks, per_zone * columns),
    )


def per_device(gate_source, up_source, down_source, source_order, target_order):
    groups, shards = lax.axis_size("grp"), lax.axis_size("sub")
    sources = (gate_source, up_source, down_source)
    if groups != 8:
        return plain(*sources, source_order, target_order)
    per_zone = 2 * gate_source.shape[0]
    table, choice = plan(source_order, target_order, per_zone)

    def routed(number, cap, edge):
        def run(table, sources):
            return line(cap, edge, number, per_zone, shards, table, sources)

        return run

    cases = CASES + ((2 * per_zone, per_zone),)
    branches = [routed(i, *case) for i, case in enumerate(cases)]
    return lax.switch(choice[0], branches, table, sources)


def solution(mesh):
    placed = (P("grp", "sub", None), P("grp", "sub", None), P("grp", "sub", None), P(), P())
    return jax.shard_map(
        per_device,
        mesh=mesh,
        in_specs=placed,
        out_specs=(P(None, "grp", "sub", None, None, None), P(None, "grp", "sub", None, None)),
        check_vma=False,
    )
```

```python
import functools

import jax
import jax.numpy as jnp
from jax import lax
from jax.experimental import pallas as pl
from jax.experimental.pallas import tpu as pltpu
from jax.sharding import PartitionSpec as P

BLOCK = 128
EPS = 1e-06
MESH = pl.DeviceIdType.MESH
PIECE = 16
CASES = ((6, 6), (7, 6), (7, 7), (8, 7), (8, 8), (9, 8), (10, 8), (11, 8), (12, 8))
FIRST = 2
LAST = 1
LEAD = 3
HOLD = 16
LASTS = 20
ARRIVE = 12
LOADS = 3
TURNS = 4
RING = 6
TURN_AT = 3
LAG_IN = 2
LAG_OUT = 10


def pick(source_order, target_order):
    matches = source_order[None, :] == target_order[:, None]
    slots = jnp.arange(source_order.shape[0], dtype=jnp.int32)
    return jnp.sum(jnp.where(matches, slots[None, :], 0), axis=1, dtype=jnp.int32)


def plain(gate_source, up_source, down_source, source_order, target_order):
    stacked = jnp.stack([gate_source, up_source, down_source])
    matrices, local_slots, local_rows, hidden = stacked.shape
    groups = lax.axis_size("grp")
    shards = lax.axis_size("sub")
    devices = groups * shards
    experts = local_slots * groups
    full_rows = local_rows * shards
    targets = groups // 2
    per_group = experts // targets
    splits = 2 * shards
    columns = hidden // splits
    picked = pick(source_order, target_order)
    slab_rows = local_rows // devices
    pieces = stacked.reshape(matrices, 1, local_slots, devices, slab_rows, hidden)
    received = lax.all_to_all(pieces, ("grp", "sub"), split_axis=3, concat_axis=1, tiled=True)
    received = received.reshape(matrices, groups, shards, local_slots, slab_rows, hidden)
    received = received.transpose(0, 1, 3, 2, 4, 5).reshape(
        matrices, experts, shards * slab_rows, hidden
    )
    ordered = jnp.take(received, picked, axis=1)
    outgoing = ordered.reshape(matrices, targets, per_group, shards * slab_rows, splits, columns)
    outgoing = outgoing.transpose(0, 1, 4, 2, 3, 5).reshape(
        matrices, devices, per_group, 1, shards * slab_rows, columns
    )
    placed = lax.all_to_all(outgoing, ("grp", "sub"), split_axis=1, concat_axis=3, tiled=True)
    placed = placed.reshape(matrices, per_group, devices, shards, slab_rows, columns)
    placed = placed.transpose(0, 1, 3, 2, 4, 5).reshape(matrices, per_group, full_rows, columns)
    num_blocks = full_rows // BLOCK
    blocks = placed.astype(jnp.float32).reshape(matrices, per_group, num_blocks, BLOCK, columns)
    block_scale = jnp.max(jnp.abs(blocks), axis=3) + EPS
    quantized = (blocks / block_scale[:, :, :, None, :]).astype(jnp.bfloat16)
    quantized = quantized.reshape(matrices, per_group, full_rows, columns).transpose(0, 1, 3, 2)
    quantized = quantized.reshape(matrices, 1, 1, per_group, columns, full_rows)
    block_scale = block_scale.transpose(0, 2, 1, 3).reshape(
        matrices, 1, 1, num_blocks, per_group * columns
    )
    return (quantized, block_scale)


def plan_kernel(per_zone, source_order, target_order, table, choice, goes):
    experts = source_order.shape[0]
    spare = table.shape[0] - 1
    zone = lax.axis_index("grp") // 2
    i32 = jnp.int32

    def outer(z):
        return (z == 0) | (z == 3)

    def clear(i, _):
        table[i] = 0
        return 0

    lax.fori_loop(0, spare + 1, clear, 0, unroll=True)

    def note(j, _):
        goes[target_order[j]] = j
        return 0

    lax.fori_loop(0, experts, note, 0, unroll=True)

    def route(p, counts):
        in0, in3, out0, out3, first0, first1, last0, last1, rest0, rest1 = counts
        target = goes[source_order[p]]
        here, there, own = p // per_zone, target // per_zone, p % per_zone
        moves = here != there
        leaves = outer(here) & moves
        left = here < 2
        crosses = left != (there < 2)
        enters = outer(there) & moves
        rank_in = jnp.where(here == 0, in0, in3)
        rank_out = jnp.where(there == 0, out0, out3)
        first = jnp.where(left, first0, first1)
        final = jnp.where(left, last0, last1)
        rest = jnp.where(left, rest0, rest1)
        leads = crosses & jnp.logical_not(outer(here)) & (first < FIRST)
        trails = crosses & jnp.logical_not(leads) & jnp.logical_not(outer(there)) & (final < LAST)
        other = crosses & jnp.logical_not(leads | trails)
        seat = jnp.where(leads, first, jnp.where(trails, FIRST + final, FIRST + LAST + rest))
        on_inner = jnp.where(leaves, per_zone + rank_in, own)
        after_mid = jnp.where(crosses, 2 * per_zone + seat, on_inner)
        ends = jnp.where(moves, jnp.where(outer(there), per_zone + rank_out, after_mid), own)
        inward = leaves & (here == zone)
        table[jnp.where(inward, rank_in, spare)] = own
        outward = enters & jnp.logical_not(outer(zone)) & ((there < 2) == (zone < 2))
        table[jnp.where(outward, rank_out, spare)] = after_mid
        over = crosses & (left == (zone < 2))
        table[jnp.where(over, per_zone + seat, spare)] = on_inner
        stays = there == zone
        table[jnp.where(stays, 3 * per_zone + target % per_zone, spare)] = ends

        def add(flag):
            return jnp.where(flag, 1, 0).astype(i32)

        right = jnp.logical_not(left)
        return (
            in0 + add(leaves & (here == 0)),
            in3 + add(leaves & (here == 3)),
            out0 + add(enters & (there == 0)),
            out3 + add(enters & (there == 3)),
            first0 + add(leads & left),
            first1 + add(leads & right),
            last0 + add(trails & left),
            last1 + add(trails & right),
            rest0 + add(other & left),
            rest1 + add(other & right),
        )

    zero = jnp.zeros((), i32)
    counts = lax.fori_loop(0, experts, route, (zero,) * 10, unroll=True)
    beside = jnp.maximum(counts[0], counts[1])
    middle = FIRST + LAST + jnp.maximum(counts[8], counts[9])
    index = jnp.full((), len(CASES), i32)
    for i in range(len(CASES) - 1, -1, -1):
        cap, edge = CASES[i]
        index = jnp.where((middle <= cap) & (beside <= edge), i, index)
    choice[0] = index


def plan(source_order, target_order, per_zone):
    smem = pl.BlockSpec(memory_space=pltpu.SMEM)
    return pl.pallas_call(
        functools.partial(plan_kernel, per_zone),
        out_shape=(
            jax.ShapeDtypeStruct((4 * per_zone + 1,), jnp.int32),
            jax.ShapeDtypeStruct((1,), jnp.int32),
        ),
        in_specs=[smem, smem],
        out_specs=(smem, smem),
        scratch_shapes=[pltpu.SMEM(source_order.shape, jnp.int32)],
        name="plan",
    )(source_order, target_order)


def line_kernel(cap, per_zone, table, *refs):
    sources, out, kept = refs[:3], refs[3], refs[4]
    raw, turned, held, beside, lead, middle, last, near, whole = refs[5:14]
    in_sem, ex_send, ex_recv, be_send, be_recv = refs[14:19]
    le_send, le_recv, mi_send, mi_recv, la_send, la_recv = refs[19:]
    grp, sub = lax.axis_index("grp"), lax.axis_index("sub")
    zone, half = grp // 2, grp % 2
    matrices = len(sources)
    local, rows, hidden = sources[0].shape
    steps, _, shards, piece, _ = held.shape
    edge = beside.shape[1]
    splits = 2 * shards
    columns = hidden // splits
    cuts = columns // piece
    parts = rows // BLOCK
    chunks = matrices * parts
    exchanges = ex_recv.shape[0]
    me = half * shards + sub
    is_outer = (zone == 0) | (zone == 3)
    is_inner = (zone == 1) | (zone == 2)
    neighbour = (zone + 1 - 2 * (zone % 2)) * 2 + half
    across = (3 - zone) * 2 + half

    def load(g, i):
        return pltpu.make_async_copy(
            sources[i].at[:, pl.ds(pl.multiple_of((g % parts) * BLOCK, BLOCK), BLOCK), :],
            raw.at[g % LOADS],
            in_sem.at[g % LOADS],
        )

    def start_load(g):
        for i in range(matrices):

            @pl.when(g // parts == i)
            def _():
                load(g, i).start()

    def exchange(g, c, to):
        start = pl.multiple_of(to * columns + c * piece, 16)
        return pltpu.make_async_remote_copy(
            src_ref=turned.at[g % TURNS, :, pl.ds(start, piece), :],
            dst_ref=held.at[g * cuts + c, pl.ds(half * local, local), sub],
            send_sem=ex_send.at[g % TURNS],
            recv_sem=ex_recv.at[(g * cuts + c) % exchanges],
            device_id=(zone * 2 + to // shards, to % shards),
            device_id_type=MESH,
        )

    def turn(g):
        load(g, 0).wait()

        def one(e, _):
            for b in range(hidden // BLOCK):
                turned[g % TURNS, e, b * BLOCK : (b + 1) * BLOCK, :] = raw[
                    g % LOADS, e, :, b * BLOCK : (b + 1) * BLOCK
                ].T
            return 0

        lax.fori_loop(0, local, one, 0, unroll=True)

        @pl.when(g + LOADS < chunks)
        def _():
            start_load(g + LOADS)

    def start_exchange(g):
        def cut(c, _):
            start = pl.multiple_of(me * columns + c * piece, 16)
            pltpu.make_async_copy(
                turned.at[g % TURNS, :, pl.ds(start, piece), :],
                held.at[g * cuts + c, pl.ds(half * local, local), sub],
                ex_recv.at[(g * cuts + c) % exchanges],
            ).start()

            def go(d, _):
                exchange(g, c, lax.rem(me + d, splits)).start()
                return 0

            return lax.fori_loop(1, splits, go, 0)

        lax.fori_loop(0, cuts, cut, 0)

    def wait_exchange(j):
        mine = held.at[j, pl.ds(0, per_zone)]
        pltpu.make_async_copy(mine, mine, ex_recv.at[j % exchanges]).wait()

    def gather(j, work, *ranges):
        for slots in ranges:
            for i in slots:
                work[i] = held[j, i]

    def wait_turned(slot):
        sent = turned.at[slot, :, pl.ds(0, (splits - 1) * columns), :]
        pltpu.make_async_copy(sent, sent, ex_send.at[slot]).wait()

    def send_beside(j):
        return pltpu.make_async_remote_copy(
            src_ref=beside.at[j % RING], dst_ref=held.at[j, pl.ds(per_zone, edge)],
            send_sem=be_send.at[j % RING], recv_sem=be_recv.at[j % ARRIVE],
            device_id=(neighbour, sub), device_id_type=MESH,
        )

    at_lead = 2 * per_zone
    at_last = at_lead + FIRST
    at_rest = at_last + LAST

    def send_across(j, ref, depth, start, send_sem, recv_sem):
        return pltpu.make_async_remote_copy(
            src_ref=ref.at[j % depth], dst_ref=held.at[j, pl.ds(start, ref.shape[1])],
            send_sem=send_sem.at[j % depth], recv_sem=recv_sem.at[j % recv_sem.shape[0]],
            device_id=(across, sub), device_id_type=MESH,
        )

    def send_lead(j):
        return send_across(j, lead, RING, at_lead, le_send, le_recv)

    def send_middle(j):
        return send_across(j, middle, RING, at_rest, mi_send, mi_recv)

    def send_last(j):
        return send_across(j, last, LASTS, at_last, la_send, la_recv)

    def put_beside(j, work):
        @pl.when(j >= RING)
        def _():
            send_beside(j - RING).wait_send()

        def put(k, _):
            beside[j % RING, k] = work[table[k]]
            return 0

        lax.fori_loop(0, edge, put, 0, unroll=True)
        send_beside(j).start()

    def put_across(j, ref, depth, send, start):
        @pl.when(j >= depth)
        def _():
            send(j - depth).wait_send()

        for k in range(ref.shape[1]):
            ref[j % depth, k] = near[table[per_zone + start - at_lead + k]]

    def finish(j):
        m, q, c = j // (parts * cuts), (j // cuts) % parts, j % cuts
        unit = pl.ds(pl.multiple_of(c * piece, piece), piece)
        lanes = lax.broadcasted_iota(jnp.int32, (piece, BLOCK), 1)

        def one(k, _):
            x = whole[table[3 * per_zone + k]].astype(jnp.float32)
            scale = jnp.max(jnp.abs(x), axis=2, keepdims=True) + EPS
            y = (x * (1.0 / scale)).astype(jnp.bfloat16)
            seen = jnp.where(q == 0, 0.0, kept[m, k, unit, :])
            for s in range(shards):
                start = pl.multiple_of(s * rows + q * BLOCK, BLOCK)
                out[m, k, unit, pl.ds(start, BLOCK)] = y[s]
                seen = jnp.where(lanes == s * parts + q, scale[s], seen)
            kept[m, k, unit, :] = seen
            return 0

        lax.fori_loop(0, per_zone, one, 0, unroll=True)

    start_load(jnp.int32(0))
    barrier = pltpu.get_barrier_semaphore()

    def greet(d, _):
        to = lax.rem(me + d, splits)
        pl.semaphore_signal(
            barrier, inc=1, device_id=(zone * 2 + to // shards, to % shards), device_id_type=MESH
        )
        return 0

    lax.fori_loop(1, splits, greet, 0)
    pl.semaphore_signal(barrier, inc=1, device_id=(neighbour, sub), device_id_type=MESH)

    @pl.when(is_inner)
    def _():
        pl.semaphore_signal(barrier, inc=1, device_id=(across, sub), device_id_type=MESH)

    for g in range(1, LOADS):
        start_load(jnp.int32(g))
    turn(jnp.int32(0))
    pl.semaphore_wait(barrier, jnp.where(is_inner, splits + 1, splits))
    start_exchange(jnp.int32(0))

    mine, both = range(per_zone), range(per_zone + edge)

    def step(u, _):
        @pl.when(is_outer)
        def _():
            @pl.when(u < steps)
            def _():
                wait_exchange(u)
                gather(u, near, mine)
                put_beside(u, near)

            f = u - LAG_OUT

            @pl.when((f >= 0) & (f < steps))
            def _():
                send_beside(f).wait_recv()
                gather(f, whole, both)
                finish(f)

        @pl.when(is_inner)
        def _():
            @pl.when(u < steps)
            def _():
                wait_exchange(u)
                gather(u, near, mine)
                put_across(u, lead, RING, send_lead, at_lead)
                send_lead(u).start()

            t = u - LEAD

            @pl.when((t >= 0) & (t < steps))
            def _():
                send_beside(t).wait_recv()
                gather(t, near, both)
                put_across(t, middle, RING, send_middle, at_rest)
                send_middle(t).start()
                put_across(t, last, LASTS, send_last, at_last)

                @pl.when(t >= HOLD)
                def _():
                    send_last(t - HOLD).start()

                @pl.when(t == steps - 1)
                def _():
                    def go(j, _):
                        send_last(j).start()
                        return 0

                    lax.fori_loop(steps - HOLD, steps, go, 0)

            i = t - LAG_IN

            @pl.when((i >= 0) & (i < steps))
            def _():
                send_lead(i).wait_recv()
                send_middle(i).wait_recv()
                gather(i, whole, both, range(at_lead, at_last), range(at_rest, at_lead + cap))
                put_beside(i, whole)

            f = i - HOLD

            @pl.when((f >= 0) & (f < steps))
            def _():
                send_last(f).wait_recv()
                gather(f, whole, both, range(at_lead, at_lead + cap))
                finish(f)

        g = u // cuts + 1

        @pl.when((u % cuts == TURN_AT) & (g < chunks))
        def _():
            @pl.when(g >= TURNS)
            def _():
                wait_turned(g % TURNS)

            turn(g)
            start_exchange(g)

        return 0

    lax.fori_loop(0, steps + max(LAG_OUT, LEAD + LAG_IN + HOLD), step, 0)
    for j in range(TURNS):
        wait_turned(j)
    for j in range(steps - RING, steps):
        send_beside(jnp.int32(j)).wait_send()

    @pl.when(is_inner)
    def _():
        for j in range(steps - RING, steps):
            send_lead(jnp.int32(j)).wait_send()
            send_middle(jnp.int32(j)).wait_send()
        for j in range(steps - LASTS, steps):
            send_last(jnp.int32(j)).wait_send()


def tail_kernel(values, kept, packed, scales, ready, sems, sem):
    matrices, per_zone, columns, _ = values.shape

    def write(i):
        m, k = i // per_zone, i % per_zone
        return pltpu.make_async_copy(values.at[m, k], packed.at[m, k], sems.at[0])

    for i in range(matrices * per_zone):
        write(i).start()
    for m in range(matrices):
        for k in range(per_zone):
            ready[m, :, k * columns : (k + 1) * columns] = kept[m, k].T[: ready.shape[1], :]
    last = pltpu.make_async_copy(ready, scales, sem)
    last.start()
    pltpu.make_async_copy(values, packed, sems.at[0]).wait()
    last.wait()


def line(cap, edge, number, per_zone, shards, table, sources):
    local, rows, hidden = sources[0].shape
    columns = hidden // (2 * shards)
    matrices, full = len(sources), rows * shards
    blocks = full // BLOCK
    steps = matrices * (rows // BLOCK) * (columns // PIECE)
    rest = cap - FIRST - LAST
    bf16, f32 = jnp.bfloat16, jnp.float32
    slot = (shards, PIECE, BLOCK)
    dma = pltpu.SemaphoreType.DMA
    slots = (steps + 1) * (2 * per_zone + cap) + 2 * per_zone
    slots += RING * (edge + FIRST + rest) + LASTS * LAST
    room = 2 * (slots * shards * PIECE * BLOCK + (LOADS + TURNS) * local * BLOCK * hidden)
    anywhere = pl.BlockSpec(memory_space=pl.ANY)
    vmem = pl.BlockSpec(memory_space=pltpu.VMEM)
    values, kept = pl.pallas_call(
        functools.partial(line_kernel, cap, per_zone),
        out_shape=(
            pltpu.VMEM((matrices, per_zone, columns, full), bf16),
            pltpu.VMEM((matrices, per_zone, columns, BLOCK), f32),
        ),
        in_specs=[pl.BlockSpec(memory_space=pltpu.SMEM)] + [anywhere] * matrices,
        out_specs=(vmem, vmem),
        scratch_shapes=[
            pltpu.VMEM((LOADS, local, BLOCK, hidden), bf16),
            pltpu.VMEM((TURNS, local, hidden, BLOCK), bf16),
            pltpu.VMEM((steps, 2 * per_zone + cap) + slot, bf16),
            pltpu.VMEM((RING, edge) + slot, bf16),
            pltpu.VMEM((RING, FIRST) + slot, bf16),
            pltpu.VMEM((RING, rest) + slot, bf16),
            pltpu.VMEM((LASTS, LAST) + slot, bf16),
            pltpu.VMEM((2 * per_zone,) + slot, bf16),
            pltpu.VMEM((2 * per_zone + cap,) + slot, bf16),
            dma((LOADS,)),
            dma((TURNS,)),
            dma((3 * columns // PIECE,)),
            dma((RING,)),
            dma((ARRIVE,)),
            dma((RING,)),
            dma((ARRIVE,)),
            dma((RING,)),
            dma((ARRIVE,)),
            dma((LASTS,)),
            dma((HOLD + 8,)),
        ],
        compiler_params=pltpu.CompilerParams(
            has_side_effects=True, collective_id=number, vmem_limit_bytes=room + 2**20
        ),
        name=f"line_{cap}_{edge}",
    )(table, *sources)
    packed, scales = pl.pallas_call(
        tail_kernel,
        out_shape=(
            jax.ShapeDtypeStruct(values.shape, bf16),
            jax.ShapeDtypeStruct((matrices, blocks, per_zone * columns), f32),
        ),
        in_specs=[vmem, vmem],
        out_specs=(anywhere, anywhere),
        scratch_shapes=[
            pltpu.VMEM((matrices, blocks, per_zone * columns), f32),
            dma((1,)),
            dma(()),
        ],
        compiler_params=pltpu.CompilerParams(vmem_limit_bytes=2**22),
        name="tail",
    )(
        pltpu.with_memory_space_constraint(values, pltpu.VMEM),
        pltpu.with_memory_space_constraint(kept, pltpu.VMEM),
    )
    return (
        packed.reshape(matrices, 1, 1, per_zone, columns, full),
        scales.reshape(matrices, 1, 1, blocks, per_zone * columns),
    )


def per_device(gate_source, up_source, down_source, source_order, target_order):
    groups, shards = lax.axis_size("grp"), lax.axis_size("sub")
    sources = (gate_source, up_source, down_source)
    if groups != 8:
        return plain(*sources, source_order, target_order)
    per_zone = 2 * gate_source.shape[0]
    table, choice = plan(source_order, target_order, per_zone)

    def routed(number, cap, edge):
        def run(table, sources):
            return line(cap, edge, number, per_zone, shards, table, sources)

        return run

    cases = CASES + ((2 * per_zone, per_zone),)
    branches = [routed(i, *case) for i, case in enumerate(cases)]
    return lax.switch(choice[0], branches, table, sources)


def solution(mesh):
    placed = (P("grp", "sub", None), P("grp", "sub", None), P("grp", "sub", None), P(), P())
    return jax.shard_map(
        per_device,
        mesh=mesh,
        in_specs=placed,
        out_specs=(P(None, "grp", "sub", None, None, None), P(None, "grp", "sub", None, None)),
        check_vma=False,
    )
```
